32 devices in a mesh: prow: 4 (over y, core), pcol: 8 (over z, x).
Axes of the slice: x: 2, y: 2, z: 4, core: 2. Of those that a mesh axis runs over, the one named last changes fastest.
Arguments:
- diag_block: float32 [512, 512], P(('prow', 'pcol')), as said below
- panel: float32 [4, 2048, 512], P(None, ('prow', 'pcol')), may hold values from -2.4 to 2.4
- trailing: float32 [4, 2048, 2, 4096], P(None, 'prow', None, 'pcol'), may hold values from -6 to 6
Outputs:
- factor_diag: float32 [512, 512], P(('prow', 'pcol'))
- factor_panel: float32 [4, 2048, 512], P(None, ('prow', 'pcol'))
- updated: float32 [4, 2048, 2, 4096], P(None, 'prow', None, 'pcol')
The draws below stay inside these ranges and needn't reach their ends.
Inputs may be any that keep to these rules, and one draw needn't show every extreme that they name: diag_block is symmetric positive definite with eigenvalues of at least 1.
All inputs are finite; a program needn't handle non-finite values.
Results may differ from the reference program's by a relative error of at most 0.0003.
Values sent between devices are 32-bit elements; how exact they have to be, the bound alone decides.
No kernel may reach another device: no remote copies, remote signals or barrier semaphores. Data moves between devices by JAX's collectives and lax.ppermute only.
A program may use at most 128 MiB of HBM per device.

```python
import jax
import jax.numpy as jnp
from jax import lax

B = 512
RBLK = 16
N_PROW = 4
N_PCOL = 8


def draw_diag_block(key, part):
    inner = jax.random.fold_in(key, 7)
    matrix = jax.random.normal(inner, (B, B), jnp.float32)
    matrix = matrix / jnp.sqrt(jnp.float32(B))
    return jnp.dot(matrix, matrix.T, precision=lax.Precision.HIGHEST) + jnp.eye(B, dtype=jnp.float32)


def levels(key, extent, pieces, low, largest):
    factor_of, own = 1.0, jax.random.fold_in(key, 6)
    for position, shards_of in pieces:
        heights = jnp.exp(jax.random.uniform(jax.random.fold_in(own, position), (shards_of,), jnp.float32, low / len(pieces), largest / len(pieces)))
        factor_of = factor_of * jnp.repeat(heights, extent[position] // shards_of).reshape([-1 if axis == position else 1 for axis in range(len(extent))])
    return factor_of


def centred(rng, shape, scale, bound, split=(), kind=jnp.bfloat16):
    result = jax.random.normal(rng, shape, jnp.float32) * scale
    if len(split) > 0:
        result = levels(rng, shape, split, -0.22, 0.18) * result
    return jnp.clip(result, min=-bound, max=bound).astype(kind)


def setup_inputs(seed: int = 0) -> dict:
    key_list = jax.random.split(jax.random.key(seed), 4)
    return {
        "diag_block": draw_diag_block(jax.random.fold_in(key_list[3], 71), 0),
        "panel": centred(key_list[1], (RBLK // N_PROW, N_PROW * B, B), 0.3, 2.4, ((1, 32),), jnp.float32),
        "trailing": centred(key_list[2], (RBLK // N_PROW, N_PROW * B, RBLK // N_PCOL, N_PCOL * B), 1.0, 6.0, ((1, 4), (3, 8)), jnp.float32),
    }


def reference(diag_block, panel, trailing):
    lower = jnp.linalg.cholesky(diag_block)
    rows = panel.reshape(-1, B)
    solved = jax.scipy.linalg.solve_triangular(lower, rows.T, lower=True).T
    blocks = solved.reshape(RBLK, B, B)
    whole = trailing.reshape(RBLK, B, RBLK, B)
    columns = jnp.arange(RBLK, dtype=jnp.int32)

    def one_row(index):
        left = lax.dynamic_index_in_dim(blocks, index, 0, keepdims=False)
        block_row = lax.dynamic_index_in_dim(whole, index, 0, keepdims=False)
        present = (columns <= index).astype(jnp.float32)
        product = jnp.einsum('ik,sjk->isj', left, blocks, precision=lax.Precision.HIGHEST)
        return block_row - present[None, :, None] * product
    updated = lax.map(one_row, jnp.arange(RBLK, dtype=jnp.int32))
    return (lower, solved.reshape(panel.shape), updated.reshape(trailing.shape))
```

```python
import jax
import jax.numpy as jnp
from jax import lax
from jax.experimental import pallas as pl
from jax.experimental.pallas import tpu as pltpu
from jax.sharding import PartitionSpec as P


AXES = ("prow", "pcol")
NT = (((1,), (1,)), ((), ()))
NN = (((1,), (0,)), ((), ()))
BLK = 128
GRP = 8


def fdot(a, b, dims):
    return lax.dot_general(a, b, dims, precision=lax.Precision.HIGHEST, preferred_element_type=jnp.float32)


def split(x):
    high = x.astype(jnp.bfloat16)
    return high, (x - high.astype(jnp.float32)).astype(jnp.bfloat16)


def dot3(a, b):
    def one(x, y):
        return lax.dot_general(x, y, NT, preferred_element_type=jnp.float32)
    return one(a[0], b[0]) + (one(a[0], b[1]) + one(a[1], b[0]))


def eliminate(s_ref, i_ref):
    full = (GRP, BLK)
    sub = lax.broadcasted_iota(jnp.int32, full, 0)
    lane = lax.broadcasted_iota(jnp.int32, full, 1)

    def row(x, k):
        return jnp.broadcast_to(x[k:k + 1, :], full)

    def col(x, k):
        return jnp.broadcast_to(x[:, k:k + 1], full)

    for g in range(BLK // GRP):
        at = g * GRP
        s8 = s_ref[at:at + GRP, :]
        i8 = i_ref[at:at + GRP, :]
        c = [col(s8, at + m) for m in range(GRP)]
        recip, cross, srow, irow = [], {}, [], []
        scale = jnp.zeros(full, jnp.float32)
        for k in range(GRP):
            pivot = row(c[k], k)
            t = 1.0 / pivot
            recip.append(t)
            scale = jnp.where(sub == k, lax.rsqrt(pivot), scale)
            w = jnp.where(sub > k, c[k] * t, 0.0)
            srow.append(row(s8, k))
            irow.append(row(i8, k))
            for m in range(k + 1, GRP):
                cross[k, m] = row(c[k], m)
                c[m] = c[m] - w * cross[k, m]
            s8 = s8 - w * srow[k]
            i8 = i8 - w * irow[k]
        s_ref[at:at + GRP, :] = jnp.where(lane >= sub + at, s8 * scale, 0.0)
        i_ref[at:at + GRP, :] = i8 * scale
        for h in range(g + 1, BLK // GRP):
            to = h * GRP
            sh = s_ref[to:to + GRP, :]
            ih = i_ref[to:to + GRP, :]
            ch = [col(sh, at + m) for m in range(GRP)]
            for k in range(GRP):
                w = ch[k] * recip[k]
                for m in range(k + 1, GRP):
                    ch[m] = ch[m] - w * cross[k, m]
                sh = sh - w * srow[k]
                ih = ih - w * irow[k]
            s_ref[to:to + GRP, :] = sh
            i_ref[to:to + GRP, :] = ih


def factor_kernel(slots, parts, l_ref, own_ref, m_ref, a_ref, s_ref, i_ref):
    width = a_ref.shape[0]
    rows = own_ref.shape[0]
    steps = width // BLK
    step = pl.program_id(0)

    @pl.when(step == 0)
    def _():
        for k in range(parts.shape[0]):
            at = pl.multiple_of(slots[k] * rows, 8)
            a_ref[pl.ds(at, parts.shape[1]), :] = parts[k]
        l_ref[...] = jnp.zeros_like(l_ref)
        m_ref[...] = jnp.zeros_like(m_ref)

    eye = (lax.broadcasted_iota(jnp.int32, (BLK, BLK), 0)
           == lax.broadcasted_iota(jnp.int32, (BLK, BLK), 1)).astype(jnp.float32)
    for b in range(steps):
        @pl.when(step == b)
        def _(b=b):
            s_ref[...] = a_ref[b * BLK:(b + 1) * BLK, b * BLK:(b + 1) * BLK]
            i_ref[...] = eye

    eliminate(s_ref, i_ref)

    for b in range(steps):
        @pl.when(step == b)
        def _(b=b):
            base, end = b * BLK, (b + 1) * BLK
            inv = i_ref[...]
            l_ref[base:end, base:end] = s_ref[...].T
            if b:
                m_ref[base:end, :base] = fdot(inv, m_ref[base:end, :base], NN)
            m_ref[base:end, base:end] = inv
            if end < width:
                low = fdot(a_ref[end:, base:end], inv, NT)
                l_ref[end:, base:end] = low
                a_ref[end:, end:] = a_ref[end:, end:] - fdot(low, low, NT)
                m_ref[end:, :end] = m_ref[end:, :end] - fdot(low, m_ref[base:end, :end], NN)

    @pl.when(step == steps - 1)
    def _():
        if rows % 8 == 0:
            own_ref[...] = l_ref[pl.ds(pl.multiple_of(slots[parts.shape[0]] * rows, 8), rows), :]


def factor(slots, parts, rows):
    width = parts.shape[2]
    square = jax.ShapeDtypeStruct((width, width), jnp.float32)
    whole = pl.BlockSpec((width, width), lambda i, s: (0, 0))
    return pl.pallas_call(
        factor_kernel,
        out_shape=(square, jax.ShapeDtypeStruct((rows, width), jnp.float32), square),
        grid_spec=pltpu.PrefetchScalarGridSpec(
            num_scalar_prefetch=1,
            grid=(width // BLK,),
            in_specs=[pl.BlockSpec(parts.shape, lambda i, s: (0, 0, 0))],
            out_specs=(whole, pl.BlockSpec((rows, width), lambda i, s: (0, 0)), whole),
            scratch_shapes=[
                pltpu.VMEM((width, width), jnp.float32),
                pltpu.VMEM((BLK, BLK), jnp.float32),
                pltpu.VMEM((BLK, BLK), jnp.float32),
            ],
        ),
        name="factor",
    )(slots, parts)


def solve_rows(x, inv):
    half = x[0].shape[1] // 2
    left = dot3([t[:, :half] for t in x], [t[:half, :half] for t in inv])
    right = dot3(x, [t[half:, :] for t in inv])
    return left, right


def update_kernel(n_rows, n_cols, masks, groups, place, inv_ref, c_ref, *refs):
    units = refs[:len(masks)]
    refs = refs[len(masks):]
    n_col = sum(1 + len(g[1]) for g in groups)
    cols, refs = refs[:n_col], refs[n_col:]
    panel_out, out_ref, xs_h, xs_l, fr, inv_h, inv_l, xc, fc_h, fc_l, sem = refs
    u = pl.program_id(0)
    p, q, owner = place[0], place[1], place[2]
    rows = units[0].shape[1]
    width = inv_ref.shape[0]
    n_v = xc.shape[0]

    def copies(start):
        at = 0
        for group, others in groups:
            for j, other in enumerate((0,) + others):
                src = cols[at + j]

                @pl.when((p ^ owner) == other)
                def _(src=src, group=group):
                    for i, mask in enumerate(group):
                        for v in range(n_v):
                            dst = xc.at[v, pl.ds(pl.multiple_of((q ^ mask) * rows, 8), rows), :]
                            cp = pltpu.make_async_copy(src.at[i, v], dst, sem.at[masks.index(mask), v])
                            if start:
                                cp.start()
                            else:
                                cp.wait()
            at += 1 + len(others)

    @pl.when(u == 0)
    def _():
        copies(True)
        high, low = split(inv_ref[...])
        inv_h[...] = high
        inv_l[...] = low
        copies(False)
        for v in range(n_v):
            left, right = solve_rows(split(xc[v]), (inv_h[...], inv_l[...]))
            for at, part in ((0, left), (width // 2, right)):
                high, low = split(part)
                fc_h[v, :, at:at + width // 2] = high
                fc_l[v, :, at:at + width // 2] = low

    for mask, unit in zip(masks, units):
        at = pl.multiple_of((q ^ mask) * rows, 16)
        high, low = split(unit[0])
        xs_h[pl.ds(at, rows), :] = high
        xs_l[pl.ds(at, rows), :] = low
    left, right = solve_rows((xs_h[...], xs_l[...]), (inv_h[...], inv_l[...]))
    fr[:, :width // 2] = left
    fr[:, width // 2:] = right
    panel_out[0] = fr[pl.ds(pl.multiple_of(q * rows, 8), rows), :]
    for v in range(n_v):
        present = v * n_cols + q <= u * n_rows + p

        @pl.when(present)
        def _(v=v):
            product = dot3(split(fr[...]), (fc_h[v], fc_l[v]))
            out_ref[0, :, v, :] = c_ref[0, :, v, :] - product

        @pl.when(jnp.logical_not(present))
        def _(v=v):
            out_ref[0, :, v, :] = c_ref[0, :, v, :]


def update(place, inv, trailing, units, masks, cols, groups, n_rows, n_cols):
    n_u, height, n_v, width = trailing.shape
    rows = units[0].shape[1]
    unit_spec = pl.BlockSpec((1, rows, width), lambda u, s: (u, 0, 0))
    block = pl.BlockSpec((1, height, n_v, width), lambda u, s: (u, 0, 0, 0))

    def body(*args):
        update_kernel(n_rows, n_cols, masks, groups, *args)

    return pl.pallas_call(
        body,
        out_shape=(
            jax.ShapeDtypeStruct(units[0].shape, jnp.float32),
            jax.ShapeDtypeStruct(trailing.shape, jnp.float32),
        ),
        grid_spec=pltpu.PrefetchScalarGridSpec(
            num_scalar_prefetch=1,
            grid=(n_u,),
            in_specs=[pl.BlockSpec((width, width), lambda u, s: (0, 0)), block]
            + [unit_spec] * len(units)
            + [pl.BlockSpec(memory_space=pl.ANY)] * len(cols),
            out_specs=(unit_spec, block),
            scratch_shapes=[
                pltpu.VMEM((height, width), jnp.bfloat16),
                pltpu.VMEM((height, width), jnp.bfloat16),
                pltpu.VMEM((height, width), jnp.float32),
                pltpu.VMEM((width, width), jnp.bfloat16),
                pltpu.VMEM((width, width), jnp.bfloat16),
                pltpu.VMEM((n_v, width, width), jnp.float32),
                pltpu.VMEM((n_v, width, width), jnp.bfloat16),
                pltpu.VMEM((n_v, width, width), jnp.bfloat16),
                pltpu.SemaphoreType.DMA((len(masks), n_v)),
            ],
        ),
        name="update",
    )(place, inv, trailing, *units, *cols)


def per_device(diag_block, panel, trailing):
    own_rows, width = diag_block.shape
    n_rows = lax.axis_size("prow")
    n_cols = lax.axis_size("pcol")
    p = lax.axis_index("prow").astype(jnp.int32)
    q = lax.axis_index("pcol").astype(jnp.int32)
    ratio = n_cols // n_rows

    def move(x, p_mask, q_mask):
        pairs = [
            (i * n_cols + j, (i ^ p_mask) * n_cols + (j ^ q_mask))
            for i in range(n_rows) for j in range(n_cols)
        ]
        return lax.ppermute(x, AXES, pairs)

    def send(x, p_mask):
        pairs = [
            (j % n_rows * n_cols + j, (j % n_rows ^ p_mask) * n_cols + j)
            for j in range(n_cols)
        ]
        return lax.ppermute(x, AXES, pairs)

    far = list(range(0, n_cols, 2))
    mid = [(i, j) for i in range(0, n_rows, 2) for j in range(2)]
    stage = jnp.stack([diag_block] + [move(diag_block, 0, m) for m in far[1:]])
    stage = jnp.stack([stage] + [move(stage, i, j) for i, j in mid[1:]])
    stage = jnp.stack([stage, move(stage, 1, 0)])
    parts = stage.reshape(-1, own_rows, width)
    order = [(i | c, j | m) for c in range(2) for i, j in mid for m in far]
    slots = jnp.stack([(p ^ i) * n_cols + (q ^ j) for i, j in order] + [p * n_cols + q])

    unit = {0: panel}
    for mask in far[1:]:
        low = mask & -mask
        unit[mask] = move(unit[mask ^ low], 0, low)
    for mask in far:
        unit[mask | 1] = move(unit[mask], 0, 1)
    masks = tuple(range(n_cols))

    def chosen(x):
        grouped = x.reshape((-1, ratio) + x.shape[1:])
        return lax.dynamic_index_in_dim(grouped, q // n_rows, 1, keepdims=False)

    arrival = [0] + [m for pair in zip([f | 1 for f in far], far[1:]) for m in pair] + [far[-1] | 1]
    bundles = [arrival[:1]] + [arrival[i:i + 2] for i in range(1, len(arrival), 2)]
    others = tuple(range(1, n_rows))
    cols, groups = [], []
    for bundle in bundles:
        piece = jnp.stack([chosen(unit[m]) for m in bundle])
        cols += [piece] + [send(piece, m) for m in others]
        groups.append((tuple(bundle), others))

    if own_rows % 8 == 0:
        _, factor_diag, inv = factor(slots, parts, own_rows)
    else:
        whole = jnp.zeros_like(parts).at[slots[:-1]].set(parts).reshape(1, width, width)
        lower, _, inv = factor(jnp.zeros((2,), jnp.int32), whole, own_rows)
        factor_diag = lax.dynamic_slice_in_dim(lower, slots[-1] * own_rows, own_rows, 0)
    place = jnp.stack([p, q, q % n_rows])
    factor_panel, updated = update(
        place, inv, trailing, [unit[m] for m in masks], masks, cols, tuple(groups), n_rows, n_cols
    )
    return (factor_diag, factor_panel, updated)


def solution(mesh):
    return jax.shard_map(
        per_device,
        mesh=mesh,
        in_specs=(
            P(AXES, None),
            P(None, AXES, None),
            P(None, "prow", None, "pcol"),
        ),
        out_specs=(
            P(AXES, None),
            P(None, AXES, None),
            P(None, "prow", None, "pcol"),
        ),
        check_vma=False,
    )
```

```python
import jax
import jax.numpy as jnp
from jax import lax
from jax.experimental import pallas as pl
from jax.experimental.pallas import tpu as pltpu
from jax.sharding import PartitionSpec as P


AXES = ("prow", "pcol")
NT = (((1,), (1,)), ((), ()))
NN = (((1,), (0,)), ((), ()))
BLK = 128
GRP = 8
LIMIT = 24 << 20
LOCAL = pl.BlockSpec(memory_space=pltpu.VMEM)


def fdot(a, b, dims):
    return lax.dot_general(a, b, dims, precision=lax.Precision.HIGHEST, preferred_element_type=jnp.float32)


def split(x):
    high = x.astype(jnp.bfloat16)
    return high, (x - high.astype(jnp.float32)).astype(jnp.bfloat16)


def dot3(a, b):
    def one(x, y):
        return lax.dot_general(x, y, NT, preferred_element_type=jnp.float32)

    return one(a[0], b[0]) + (one(a[0], b[1]) + one(a[1], b[0]))


def eliminate(s_ref, i_ref):
    full = (GRP, BLK)
    sub = lax.broadcasted_iota(jnp.int32, full, 0)
    lane = lax.broadcasted_iota(jnp.int32, full, 1)

    def row(x, k):
        return jnp.broadcast_to(x[k:k + 1, :], full)

    def col(x, k):
        return jnp.broadcast_to(x[:, k:k + 1], full)

    for g in range(BLK // GRP):
        at = g * GRP
        s8 = s_ref[at:at + GRP, :]
        i8 = i_ref[at:at + GRP, :]
        c = [col(s8, at + m) for m in range(GRP)]
        recip, cross, srow, irow = [], {}, [], []
        scale = jnp.zeros(full, jnp.float32)
        for k in range(GRP):
            pivot = row(c[k], k)
            t = 1.0 / pivot
            recip.append(t)
            scale = jnp.where(sub == k, lax.rsqrt(pivot), scale)
            w = jnp.where(sub > k, c[k] * t, 0.0)
            srow.append(row(s8, k))
            irow.append(row(i8, k))
            for m in range(k + 1, GRP):
                cross[k, m] = row(c[k], m)
                c[m] = c[m] - w * cross[k, m]
            s8 = s8 - w * srow[k]
            i8 = i8 - w * irow[k]
        s_ref[at:at + GRP, :] = jnp.where(lane >= sub + at, s8 * scale, 0.0)
        i_ref[at:at + GRP, :] = i8 * scale
        for h in range(g + 1, BLK // GRP):
            to = h * GRP
            sh = s_ref[to:to + GRP, :]
            ih = i_ref[to:to + GRP, :]
            ch = [col(sh, at + m) for m in range(GRP)]
            for k in range(GRP):
                w = ch[k] * recip[k]
                for m in range(k + 1, GRP):
                    ch[m] = ch[m] - w * cross[k, m]
                sh = sh - w * srow[k]
                ih = ih - w * irow[k]
            s_ref[to:to + GRP, :] = sh
            i_ref[to:to + GRP, :] = ih


def start_block(a_ref, base, s_ref, i_ref):
    s_ref[...] = a_ref[base:base + BLK, base:base + BLK]
    i_ref[...] = (lax.broadcasted_iota(jnp.int32, (BLK, BLK), 0)
                  == lax.broadcasted_iota(jnp.int32, (BLK, BLK), 1)).astype(jnp.float32)


def finish_block(a_ref, l_ref, m_ref, base, left, s_ref, i_ref):
    size = a_ref.shape[0]
    end = base + BLK
    inv = i_ref[...]
    l_ref[base:end, base:end] = s_ref[...].T
    if left + base:
        m_ref[base:end, :left + base] = fdot(inv, m_ref[base:end, :left + base], NN)
    m_ref[base:end, left + base:left + end] = inv
    if end < size:
        low = fdot(a_ref[end:, base:end], inv, NT)
        l_ref[end:, base:end] = low
        a_ref[end:, end:] = a_ref[end:, end:] - fdot(low, low, NT)
        m_ref[end:, :left + end] = m_ref[end:, :left + end] - fdot(low, m_ref[base:end, :left + end], NN)


def first_kernel(slots, parts, a_out, l_ref, m_ref, a_ref, s_ref, i_ref):
    half = a_out.shape[0]
    step = pl.program_id(0)

    @pl.when(step == 0)
    def _():
        rows = parts.shape[1]
        for k in range(parts.shape[0]):
            a_ref[pl.ds(pl.multiple_of(slots[k] * rows, 8), rows), :] = parts[k]
        l_ref[...] = jnp.zeros_like(l_ref)
        m_ref[...] = jnp.zeros_like(m_ref)

    for b in range(half // BLK):
        pl.when(step == b)(lambda b=b: start_block(a_ref, b * BLK, s_ref, i_ref))
    eliminate(s_ref, i_ref)
    for b in range(half // BLK):
        pl.when(step == b)(lambda b=b: finish_block(a_ref, l_ref, m_ref, b * BLK, 0, s_ref, i_ref))

    @pl.when(step == half // BLK - 1)
    def _():
        a_out[...] = a_ref[half:, half:]


def second_kernel(slots, a_in, l_in, m_in, own_ref, high_ref, low_ref, a_ref, l_ref, m_ref, s_ref, i_ref):
    half = a_in.shape[0]
    rows = own_ref.shape[0]
    step = pl.program_id(0)

    @pl.when(step == 0)
    def _():
        a_ref[...] = a_in[...]
        l_ref[...] = jnp.zeros_like(l_ref)
        m_ref[:, :half] = m_in[half:, :]
        m_ref[:, half:] = jnp.zeros((half, half), jnp.float32)

    for b in range(half // BLK):
        pl.when(step == b)(lambda b=b: start_block(a_ref, b * BLK, s_ref, i_ref))
    eliminate(s_ref, i_ref)
    for b in range(half // BLK):
        pl.when(step == b)(lambda b=b: finish_block(a_ref, l_ref, m_ref, b * BLK, half, s_ref, i_ref))

    @pl.when(step == half // BLK - 1)
    def _():
        high, low = split(m_in[:half, :])
        zero = jnp.zeros((half, half), jnp.bfloat16)
        high_ref[:half, :half] = high
        low_ref[:half, :half] = low
        high_ref[:half, half:] = zero
        low_ref[:half, half:] = zero
        high, low = split(m_ref[...])
        high_ref[half:, :] = high
        low_ref[half:, :] = low
        at = slots[slots.shape[0] - 1]
        own_ref[:, :half] = l_in[pl.ds(pl.multiple_of(at, 8), rows), :]

        @pl.when(at < half)
        def _():
            own_ref[:, half:] = jnp.zeros((rows, half), jnp.float32)

        @pl.when(at >= half)
        def _():
            own_ref[:, half:] = l_ref[pl.ds(pl.multiple_of(at - half, 8), rows), :]


def factor(slots, parts, rows):
    width = parts.shape[2]
    half = width // 2
    f32 = jnp.float32
    cost = pl.CostEstimate(flops=int(1.1e10), transcendentals=0, bytes_accessed=4 * width * width)

    params = pltpu.CompilerParams(vmem_limit_bytes=LIMIT)

    def shape(*dims, dtype=f32):
        return pltpu.VMEM(dims, dtype)

    small = [pltpu.VMEM((BLK, BLK), f32)] * 2
    state = pl.pallas_call(
        first_kernel,
        out_shape=(shape(half, half), shape(width, half), shape(width, half)),
        grid_spec=pltpu.PrefetchScalarGridSpec(
            num_scalar_prefetch=1, grid=(half // BLK,),
            in_specs=[LOCAL],
            out_specs=(LOCAL,) * 3,
            scratch_shapes=[pltpu.VMEM((width, width), f32)] + small,
        ),
        cost_estimate=cost,
        compiler_params=params,
        name="first",
    )(slots, parts)
    return pl.pallas_call(
        second_kernel,
        out_shape=(shape(rows, width), shape(width, width, dtype=jnp.bfloat16), shape(width, width, dtype=jnp.bfloat16)),
        grid_spec=pltpu.PrefetchScalarGridSpec(
            num_scalar_prefetch=1, grid=(half // BLK,),
            in_specs=[LOCAL] * 3,
            out_specs=(LOCAL,) * 3,
            scratch_shapes=[pltpu.VMEM((half, half), f32)] * 2 + [pltpu.VMEM((half, width), f32)] + small,
        ),
        cost_estimate=cost,
        compiler_params=params,
        name="second",
    )(slots, *state)


def solve_rows(x, inv):
    half = x[0].shape[1] // 2
    left = dot3([t[:, :half] for t in x], [t[:half, :half] for t in inv])
    right = dot3(x, [t[half:, :] for t in inv])
    return left, right


def solve_kernel(masks, place, inv_h, inv_l, *refs):
    units = refs[:len(masks)]
    panel_out, f_h, f_l, xs_h, xs_l, fr = refs[len(masks):]
    u = pl.program_id(0)
    q = place[1]
    rows = units[0].shape[1]
    half = inv_h.shape[0] // 2
    for mask, unit in zip(masks, units):
        at = pl.multiple_of((q ^ mask) * rows, 16)
        high, low = split(unit[u])
        xs_h[pl.ds(at, rows), :] = high
        xs_l[pl.ds(at, rows), :] = low
    for at, part in zip((0, half), solve_rows((xs_h[...], xs_l[...]), (inv_h[...], inv_l[...]))):
        fr[:, at:at + half] = part
        high, low = split(part)
        f_h[u, :, at:at + half] = high
        f_l[u, :, at:at + half] = low
    panel_out[0] = fr[pl.ds(pl.multiple_of(q * rows, 8), rows), :]


def solve(place, inv, units, masks):
    n_u, rows, width = units[0].shape
    height = rows * len(units)
    pair = pltpu.VMEM((n_u, height, width), jnp.bfloat16)

    def body(*args):
        solve_kernel(masks, *args)

    return pl.pallas_call(
        body,
        out_shape=(jax.ShapeDtypeStruct(units[0].shape, jnp.float32), pair, pair),
        grid_spec=pltpu.PrefetchScalarGridSpec(
            num_scalar_prefetch=1,
            grid=(n_u,),
            in_specs=[LOCAL] * (2 + len(units)),
            out_specs=(pl.BlockSpec((1, rows, width), lambda u, s: (u, 0, 0)), LOCAL, LOCAL),
            scratch_shapes=[
                pltpu.VMEM((height, width), jnp.bfloat16),
                pltpu.VMEM((height, width), jnp.bfloat16),
                pltpu.VMEM((height, width), jnp.float32),
            ],
        ),
        cost_estimate=pl.CostEstimate(flops=int(5e9), transcendentals=0, bytes_accessed=int(9e6)),
        compiler_params=pltpu.CompilerParams(vmem_limit_bytes=LIMIT),
        name="solve",
    )(place, *inv, *units)


def update_kernel(n_rows, n_cols, groups, place, inv_h, inv_l, f_h, f_l, c_ref, *refs):
    cols, refs = refs[:2 * len(groups)], refs[2 * len(groups):]
    out_ref, xs_h, xs_l, fc_h, fc_l = refs
    u = pl.program_id(0)
    p, q, owner = place[0], place[1], place[2]
    half = inv_h.shape[0] // 2
    n_v = xs_h.shape[0]
    rows = cols[0].shape[2]

    @pl.when(u == 0)
    def _():
        for j, group in enumerate(groups):
            for side in range(2):
                @pl.when(((p ^ owner) & 1) == side)
                def _(src=cols[2 * j + side], group=group):
                    for i, mask in enumerate(group):
                        at = pl.multiple_of((q ^ mask) * rows, 16)
                        for v in range(n_v):
                            high, low = split(src[i, v])
                            xs_h[v, pl.ds(at, rows), :] = high
                            xs_l[v, pl.ds(at, rows), :] = low
        for v in range(n_v):
            solved = solve_rows((xs_h[v], xs_l[v]), (inv_h[...], inv_l[...]))
            for at, part in zip((0, half), solved):
                high, low = split(part)
                fc_h[v, :, at:at + half] = high
                fc_l[v, :, at:at + half] = low

    for v in range(n_v):
        present = v * n_cols + q <= u * n_rows + p

        @pl.when(present)
        def _(v=v):
            product = dot3((f_h[u], f_l[u]), (fc_h[v], fc_l[v]))
            out_ref[0, :, v, :] = c_ref[u, :, v, :] - product

        @pl.when(jnp.logical_not(present))
        def _(v=v):
            out_ref[0, :, v, :] = c_ref[u, :, v, :]


def update(place, inv, f, trailing, cols, groups, n_rows, n_cols):
    n_u, height, n_v, width = trailing.shape
    square = pltpu.VMEM((n_v, width, width), jnp.bfloat16)

    def body(*args):
        update_kernel(n_rows, n_cols, groups, *args)

    return pl.pallas_call(
        body,
        out_shape=jax.ShapeDtypeStruct(trailing.shape, jnp.float32),
        grid_spec=pltpu.PrefetchScalarGridSpec(
            num_scalar_prefetch=1,
            grid=(n_u,),
            in_specs=[LOCAL] * (5 + len(cols)),
            out_specs=pl.BlockSpec((1, height, n_v, width), lambda u, s: (u, 0, 0, 0)),
            scratch_shapes=[square] * 4,
        ),
        compiler_params=pltpu.CompilerParams(vmem_limit_bytes=LIMIT),
        name="update",
    )(place, *inv, *f, trailing, *cols)


def per_device(diag_block, panel, trailing):
    own_rows, width = diag_block.shape
    n_rows = lax.axis_size("prow")
    n_cols = lax.axis_size("pcol")
    p = lax.axis_index("prow").astype(jnp.int32)
    q = lax.axis_index("pcol").astype(jnp.int32)
    ratio = n_cols // n_rows
    owner = q % n_rows

    def move(x, p_mask, q_mask):
        pairs = [
            (i * n_cols + j, (i ^ p_mask) * n_cols + (j ^ q_mask))
            for i in range(n_rows) for j in range(n_cols)
        ]
        return lax.ppermute(x, AXES, pairs)

    def send(x, p_mask):
        pairs = [
            (j % n_rows * n_cols + j, (j % n_rows ^ p_mask) * n_cols + j)
            for j in range(n_cols)
        ]
        return lax.ppermute(x, AXES, pairs)

    far = list(range(0, n_cols, 2))
    mid = [(i, j) for i in range(0, n_rows, 2) for j in range(2)]
    stage = jnp.stack([diag_block] + [move(diag_block, 0, m) for m in far[1:]])
    stage = jnp.stack([stage] + [move(stage, i, j) for i, j in mid[1:]])
    stage = jnp.stack([stage, move(stage, 1, 0)])
    parts = stage.reshape(-1, own_rows, width)
    order = [(i | c, j | m) for c in range(2) for i, j in mid for m in far]
    slots = [(p ^ i) * n_cols + (q ^ j) for i, j in order]
    own = (p * n_cols + q) * own_rows
    if own_rows % 8:
        parts = jnp.zeros_like(parts).at[jnp.stack(slots)].set(parts).reshape(1, width, width)
        slots = [jnp.int32(0)]

    unit = {0: panel}
    for mask in far[1:]:
        low = mask & -mask
        unit[mask] = move(unit[mask ^ low], 0, low)
    for mask in far:
        unit[mask | 1] = move(unit[mask], 0, 1)
    masks = tuple(range(n_cols))

    def chosen(x):
        grouped = x.reshape((-1, ratio) + x.shape[1:])
        return lax.dynamic_index_in_dim(grouped, q // n_rows, 1, keepdims=False)

    early = [0, 1] + [m for m in far[1:] if m & (m - 1) == 0]
    late = [far[-1] | 1]
    groups = [early, [m for m in masks if m not in early + late], late]
    cols = []
    for group in groups:
        piece = jnp.stack([chosen(unit[m]) for m in group])
        there = sum(send(piece, m) for m in range(2, n_rows, 2))
        here = jnp.where(p == owner, piece, there)
        cols += [here, move(here, 1, 0)]

    factor_diag, high, low = factor(
        jnp.stack(slots + [own // 8 * 8]), parts, max(own_rows, 8)
    )
    if own_rows % 8:
        factor_diag = lax.dynamic_slice_in_dim(factor_diag, own % 8, own_rows, 0)
    place = jnp.stack([p, q, owner])
    factor_panel, *solved = solve(place, (high, low), [unit[m] for m in masks], masks)
    updated = update(place, (high, low), solved, trailing, cols, tuple(tuple(g) for g in groups), n_rows, n_cols)
    return (factor_diag, factor_panel, updated)


def solution(mesh):
    return jax.shard_map(
        per_device,
        mesh=mesh,
        in_specs=(
            P(AXES, None),
            P(None, AXES, None),
            P(None, "prow", None, "pcol"),
        ),
        out_specs=(
            P(AXES, None),
            P(None, AXES, None),
            P(None, "prow", None, "pcol"),
        ),
        check_vma=False,
    )
```
